32 devices in a mesh: gx: 2 (over y), gz: 4 (over z), gy: 4 (over x, core).
Axes of the slice: x: 2, y: 2, z: 4, core: 2. Of those that a mesh axis runs over, the one named last changes fastest.
Arguments:
- logits: float32 [256, 131072], P('gy', ('gx', 'gz')), may hold values from -60 to 250
Outputs:
- token_potential: float32 [131072], P(('gx', 'gz'))
- expert_potential: float32 [256], P('gy')
The draws below stay inside these ranges and needn't reach their ends.
All inputs are finite; a program needn't handle non-finite values.
Results may differ from the reference program's by a relative error of at most 0.0001.
Values sent between devices are 32-bit elements; how exact they have to be, the bound alone decides.
A program may use at most 64 MiB of HBM per device.

```python
import jax
import jax.numpy as jnp

E = 256
ITERS = 3
TOKENS = 131072


def draw_logits(key, part):
    keys = jax.random.split(jax.random.fold_in(key, 11), 2)
    place = jnp.arange(TOKENS, dtype=jnp.float32) / jnp.float32(TOKENS)
    spread = (3.0 + 3.0 * place)[None, :]
    offset = jax.random.uniform(keys[1], (E, 1), jnp.float32, -1.5, 1.5)
    values = jax.random.normal(keys[0], (E, TOKENS), jnp.float32) * spread + offset
    token_ids = jnp.arange(TOKENS, dtype=jnp.int32)[None, :]
    row_ids = jnp.arange(E, dtype=jnp.int32)[:, None]
    lowest = (token_ids % 4096 == 3) & (row_ids == token_ids * 7 % E)
    values = jnp.where(lowest, -60.0, values)
    return jnp.clip(values, -60.0, 250.0).astype(jnp.float32)


def setup_inputs(seed: int = 0) -> dict:
    streams_of = jax.random.split(jax.random.key(seed), 2)
    logits = draw_logits(jax.random.fold_in(streams_of[1], 71), 0)
    return {"logits": logits}


def reference(logits):
    log_cap = jnp.log(jnp.float32(TOKENS) / jnp.float32(E))
    token_potential = jnp.zeros((TOKENS,), jnp.float32)
    expert_potential = jnp.zeros((E,), jnp.float32)
    for step in range(ITERS):
        shifted = logits + token_potential[None, :]
        top = jnp.max(shifted, axis=1)
        total = jnp.sum(jnp.exp(shifted - top[:, None]), axis=1)
        expert_potential = log_cap - (top + jnp.log(total))
        raised = logits + expert_potential[:, None]
        peak = jnp.max(raised, axis=0)
        summed = jnp.sum(jnp.exp(raised - peak[None, :]), axis=0)
        token_potential = -(peak + jnp.log(summed))
    return token_potential, expert_potential
```

```python
import functools

import jax
import jax.numpy as jnp
from jax import lax
from jax.experimental import pallas as pl
from jax.experimental.pallas import tpu as pltpu
from jax.sharding import PartitionSpec as P

ITERS = 3
LANES = 128
SUB = 8
MESH = pl.DeviceIdType.MESH


def kernel(nx, nz, ny, chunks, x_hbm, tok_ref, exp_ref, x, tops, sums, rows_out, rows_in,
           mine, theirs, peak, weight, scaled, first_tok, load_sem, es_sem, er_sem, ts_sem, tr_sem):
    experts, tokens = x.shape
    groups = experts // SUB
    blocks = tokens // LANES
    n = nx * nz
    stages = ny.bit_length() - 1
    per = blocks // chunks
    gx, gz, gy = lax.axis_index("gx"), lax.axis_index("gz"), lax.axis_index("gy")
    me = gx * nz + gz
    cap = float(tokens * n) / float(experts * ny)
    log_cap = jnp.log(jnp.full((1, LANES), cap, jnp.float32))

    loads = []
    for i in range(groups):
        rows = pl.ds(i * SUB, SUB)
        load = pltpu.make_async_copy(x_hbm.at[rows, :], x.at[rows, :], load_sem.at[i])
        load.start()
        loads.append(load)

    def peer(k):
        other = lax.rem(me + k, n)
        return (other // nz, lax.rem(other, nz), gy)

    def partner(stage):
        bit = 1 << stage
        up = lax.rem(gy // bit, 2)
        return (gx, gz, gy + bit - 2 * bit * up)

    barrier = pltpu.get_barrier_semaphore()

    def greet(k, carry):
        pl.semaphore_signal(barrier, inc=1, device_id=peer(k), device_id_type=MESH)
        return carry

    lax.fori_loop(1, n, greet, 0, unroll=n <= 8)
    for stage in range(stages):
        pl.semaphore_signal(barrier, inc=1, device_id=partner(stage), device_id_type=MESH)

    diag = (lax.broadcasted_iota(jnp.int32, (experts, LANES), 0)
            == lax.broadcasted_iota(jnp.int32, (experts, LANES), 1))

    def to_row(column):
        return jnp.sum(jnp.where(diag, jnp.broadcast_to(column, (experts, LANES)), 0.0),
                       axis=0, keepdims=True)

    def to_column(row):
        column = jnp.sum(jnp.where(diag, jnp.broadcast_to(row, (experts, LANES)), 0.0),
                         axis=1, keepdims=True)
        return jnp.broadcast_to(column, (experts, LANES))

    def exchange_rows(it, row):
        rows_out[it] = row

        def send(k, carry):
            pltpu.make_async_remote_copy(
                src_ref=rows_out.at[it], dst_ref=rows_in.at[it, k - 1],
                send_sem=es_sem.at[it], recv_sem=er_sem.at[it],
                device_id=peer(k), device_id_type=MESH).start()
            return carry

        lax.fori_loop(1, n, send, 0, unroll=n <= 8)
        whole = rows_in.at[it]
        pltpu.make_async_copy(whole, whole, er_sem.at[it]).wait()
        return [row] + [rows_in[it, k] for k in range(n - 1)]

    wide = 8 * LANES

    def fold(array, combine):
        parts = [array[:, k * LANES:(k + 1) * LANES] for k in range(array.shape[1] // LANES)]
        while len(parts) > 1:
            parts = [combine(parts[k], parts[k + 1]) for k in range(0, len(parts), 2)]
        return parts[0]

    for i in range(groups):
        rows = pl.ds(i * SUB, SUB)
        loads[i].wait()

        def higher(j, m):
            return jnp.maximum(m, x[rows, pl.ds(pl.multiple_of(j * wide, wide), wide)])

        m = fold(lax.fori_loop(1, tokens // wide, higher, x[rows, pl.ds(0, wide)], unroll=5),
                 jnp.maximum)
        tiled = jnp.concatenate([m] * 8, axis=1)

        def more(j, s):
            return s + jnp.exp(x[rows, pl.ds(pl.multiple_of(j * wide, wide), wide)] - tiled)

        s = fold(lax.fori_loop(0, tokens // wide, more, jnp.zeros((SUB, wide), jnp.float32),
                               unroll=4), jnp.add)
        tops[rows, :] = m
        sums[rows, :] = s

    lane_top = tops[...]
    top = jnp.max(lane_top, axis=1, keepdims=True)
    total = jnp.sum(sums[...] * jnp.exp(lane_top - top), axis=1, keepdims=True)
    local = to_row(top + jnp.log(total))

    pl.semaphore_wait(barrier, n - 1 + stages)

    parts = exchange_rows(0, local)
    top = functools.reduce(jnp.maximum, parts)
    total = functools.reduce(jnp.add, [jnp.exp(part - top) for part in parts])
    first_exp = log_cap - (top + jnp.log(total))
    factor = to_column(first_exp)

    def chunk(c):
        return pl.ds(c * per, per)

    def tok_copy(it, stage, c):
        return pltpu.make_async_remote_copy(
            src_ref=mine.at[it, stage, chunk(c), :], dst_ref=theirs.at[it, stage, chunk(c), :],
            send_sem=ts_sem.at[it, stage, c], recv_sem=tr_sem.at[it, stage, c],
            device_id=partner(stage), device_id_type=MESH)

    for it in range(ITERS):
        last = it == ITERS - 1
        for c in range(chunks):
            def column_pass(jj, carry):
                for u in range(SUB):
                    j = jj * SUB + u
                    lanes = pl.ds(pl.multiple_of(j * LANES, LANES), LANES)
                    if it == 0:
                        v = x[:, lanes] + factor
                        p = jnp.max(v, axis=0, keepdims=True)
                        e = jnp.exp(v - p)
                        x[:, lanes] = e
                        peak[pl.ds(j, 1), :] = p
                    else:
                        e = x[:, lanes] * factor
                    scaled[pl.ds(j, 1), :] = jnp.sum(e, axis=0, keepdims=True)
                return carry

            lax.fori_loop(c * per // SUB, (c + 1) * per // SUB, column_pass, 0)
            if it == 0:
                mine[it, 0, chunk(c), :] = peak[chunk(c), :] + jnp.log(scaled[chunk(c), :])
            else:
                mine[it, 0, chunk(c), :] = weight[chunk(c), :] * scaled[chunk(c), :]
            tok_copy(it, 0, c).start()

        acc = jnp.zeros((experts, LANES), jnp.float32)
        for stage in range(stages):
            for c in range(chunks):
                tok_copy(it, stage, c).wait_recv()
                a, b = mine[it, stage, chunk(c), :], theirs[it, stage, chunk(c), :]
                if it == 0:
                    t = jnp.maximum(a, b)
                    joined = t + jnp.log(jnp.exp(a - t) + jnp.exp(b - t))
                else:
                    joined = a + b
                if stage < stages - 1:
                    mine[it, stage + 1, chunk(c), :] = joined
                    tok_copy(it, stage + 1, c).start()
                    continue
                if last:
                    tok_ref[chunk(c), :] = first_tok[chunk(c), :] - jnp.log(joined)
                    continue
                if it == 0:
                    first_tok[chunk(c), :] = -joined
                    w = jnp.exp(peak[chunk(c), :] - joined)
                    weight[chunk(c), :] = w
                    scaled[chunk(c), :] = w
                else:
                    scaled[chunk(c), :] = weight[chunk(c), :] / joined

                def row_pass(jj, acc):
                    for u in range(SUB):
                        j = jj * SUB + u
                        lanes = pl.ds(pl.multiple_of(j * LANES, LANES), LANES)
                        acc = acc + x[:, lanes] * scaled[pl.ds(j, 1), :]
                    return acc

                acc = lax.fori_loop(c * per // SUB, (c + 1) * per // SUB, row_pass, acc)
        if not last:
            parts = exchange_rows(it + 1, to_row(jnp.sum(acc, axis=1, keepdims=True)))
            total = functools.reduce(jnp.add, parts)
            factor = to_column(cap / total)
            if it == ITERS - 2:
                exp_ref[...] = first_exp + (log_cap - jnp.log(total))

    for it in range(ITERS):
        whole = rows_in.at[it]
        pltpu.make_async_copy(whole, whole, es_sem.at[it]).wait()
        for stage in range(stages):
            for c in range(chunks):
                tok_copy(it, stage, c).wait_send()


def solution(mesh):
    nx, nz, ny = mesh.shape["gx"], mesh.shape["gz"], mesh.shape["gy"]
    n = nx * nz
    stages = ny.bit_length() - 1
    chunks = 4

    def per_device(logits):
        experts, tokens = logits.shape
        blocks = tokens // LANES
        f32 = jnp.float32
        plane = pltpu.VMEM((blocks, LANES), f32)
        tok, exp = pl.pallas_call(
            functools.partial(kernel, nx, nz, ny, chunks),
            out_shape=(jax.ShapeDtypeStruct((blocks, LANES), f32),
                       jax.ShapeDtypeStruct((1, LANES), f32)),
            in_specs=[pl.BlockSpec(memory_space=pl.ANY)],
            out_specs=(pl.BlockSpec(memory_space=pltpu.VMEM),) * 2,
            scratch_shapes=[
                pltpu.VMEM((experts, tokens), f32),
                pltpu.VMEM((experts, LANES), f32),
                pltpu.VMEM((experts, LANES), f32),
                pltpu.VMEM((ITERS, 1, LANES), f32),
                pltpu.VMEM((ITERS, n - 1, 1, LANES), f32),
                pltpu.VMEM((ITERS, stages, blocks, LANES), f32),
                pltpu.VMEM((ITERS, stages, blocks, LANES), f32),
                plane, plane, plane, plane,
                pltpu.SemaphoreType.DMA((experts // SUB,)),
                pltpu.SemaphoreType.DMA((ITERS,)),
                pltpu.SemaphoreType.DMA((ITERS,)),
                pltpu.SemaphoreType.DMA((ITERS, stages, chunks)),
                pltpu.SemaphoreType.DMA((ITERS, stages, chunks)),
            ],
            compiler_params=pltpu.CompilerParams(
                collective_id=0, has_side_effects=True, vmem_limit_bytes=60 * 1024 * 1024),
        )(logits)
        return tok.reshape(tokens), exp[0, :experts]

    return jax.shard_map(
        per_device, mesh=mesh, in_specs=(P("gy", ("gx", "gz")),),
        out_specs=(P(("gx", "gz")), P("gy")), check_vma=False)
```

```python
import functools

import jax
import jax.numpy as jnp
from jax import lax
from jax.experimental import pallas as pl
from jax.experimental.pallas import tpu as pltpu
from jax.sharding import PartitionSpec as P

ITERS = 3
LANES = 128
SUB = 8
MESH = pl.DeviceIdType.MESH


def kernel(nx, nz, ny, chunks, x_hbm, tok_ref, exp_ref, x, tops, sums, rows_out, rows_in,
           mine, theirs, held, level, weight, partial, scaled, first_tok, load_sem, es_sem, er_sem, ts_sem, tr_sem):
    experts, tokens = x.shape
    groups = experts // SUB
    blocks = tokens // LANES
    n = nx * nz
    stages = ny.bit_length() - 1
    per = blocks // chunks
    gx, gz, gy = lax.axis_index("gx"), lax.axis_index("gz"), lax.axis_index("gy")
    me = gx * nz + gz
    cap = float(tokens * n) / float(experts * ny)
    log_cap = jnp.log(jnp.full((1, LANES), cap, jnp.float32))

    loads = []
    for i in range(groups):
        rows = pl.ds(i * SUB, SUB)
        load = pltpu.make_async_copy(x_hbm.at[rows, :], x.at[rows, :], load_sem.at[i])
        load.start()
        loads.append(load)

    def peer(k):
        other = lax.rem(me + k, n)
        return (other // nz, lax.rem(other, nz), gy)

    def partner(stage):
        bit = 1 << stage
        up = lax.rem(gy // bit, 2)
        return (gx, gz, gy + bit - 2 * bit * up)

    barrier = pltpu.get_barrier_semaphore()

    def greet(k, carry):
        pl.semaphore_signal(barrier, inc=1, device_id=peer(k), device_id_type=MESH)
        return carry

    lax.fori_loop(1, n, greet, 0, unroll=n <= 8)
    for stage in range(stages):
        pl.semaphore_signal(barrier, inc=1, device_id=partner(stage), device_id_type=MESH)

    diag = (lax.broadcasted_iota(jnp.int32, (experts, LANES), 0)
            == lax.broadcasted_iota(jnp.int32, (experts, LANES), 1))

    def to_row(column):
        return jnp.sum(jnp.where(diag, jnp.broadcast_to(column, (experts, LANES)), 0.0),
                       axis=0, keepdims=True)

    def to_column(row):
        column = jnp.sum(jnp.where(diag, jnp.broadcast_to(row, (experts, LANES)), 0.0),
                         axis=1, keepdims=True)
        return jnp.broadcast_to(column, (experts, LANES))

    def exchange_rows(it, row):
        rows_out[it] = row

        def send(k, carry):
            pltpu.make_async_remote_copy(
                src_ref=rows_out.at[it], dst_ref=rows_in.at[it, k - 1],
                send_sem=es_sem.at[it], recv_sem=er_sem.at[it],
                device_id=peer(k), device_id_type=MESH).start()
            return carry

        lax.fori_loop(1, n, send, 0, unroll=n <= 8)
        whole = rows_in.at[it]
        pltpu.make_async_copy(whole, whole, er_sem.at[it]).wait()
        return [row] + [rows_in[it, k] for k in range(n - 1)]

    wide = 8 * LANES

    def pairwise(parts, combine):
        while len(parts) > 1:
            parts = [combine(*parts[k:k + 2]) if k + 1 < len(parts) else parts[k]
                     for k in range(0, len(parts), 2)]
        return parts[0]

    def fold(array, combine):
        return pairwise([array[:, k * LANES:(k + 1) * LANES]
                         for k in range(array.shape[1] // LANES)], combine)

    def tree(array, combine):
        return pairwise([array[k * SUB:(k + 1) * SUB] for k in range(groups)], combine)

    for i in range(groups):
        rows = pl.ds(i * SUB, SUB)
        loads[i].wait()

        def higher(j, m):
            return jnp.maximum(m, x[rows, pl.ds(pl.multiple_of(j * wide, wide), wide)])

        m = fold(lax.fori_loop(1, tokens // wide, higher, x[rows, pl.ds(0, wide)], unroll=5),
                 jnp.maximum)
        tiled = jnp.concatenate([m] * 8, axis=1)

        def more(j, s):
            return s + jnp.exp(x[rows, pl.ds(pl.multiple_of(j * wide, wide), wide)] - tiled)

        s = fold(lax.fori_loop(0, tokens // wide, more, jnp.zeros((SUB, wide), jnp.float32),
                               unroll=4), jnp.add)
        tops[rows, :] = m
        sums[rows, :] = s

    lane_top = tops[...]
    top = jnp.max(lane_top, axis=1, keepdims=True)
    total = jnp.sum(sums[...] * jnp.exp(lane_top - top), axis=1, keepdims=True)
    local = to_row(top + jnp.log(total))

    pl.semaphore_wait(barrier, n - 1 + stages)

    parts = exchange_rows(0, local)
    top = functools.reduce(jnp.maximum, parts)
    total = functools.reduce(jnp.add, [jnp.exp(part - top) for part in parts])
    first_exp = log_cap - (top + jnp.log(total))
    factor = to_column(first_exp)

    def chunk(c):
        return pl.ds(c * per, per)

    def tok_copy(it, stage, c):
        return pltpu.make_async_remote_copy(
            src_ref=mine.at[it, stage, chunk(c), :], dst_ref=theirs.at[it, stage, chunk(c), :],
            send_sem=ts_sem.at[it, stage, c], recv_sem=tr_sem.at[it, stage, c],
            device_id=partner(stage), device_id_type=MESH)

    for it in range(ITERS):
        last = it == ITERS - 1
        for c in range(chunks):
            def column_pass(jj, carry):
                for u in range(SUB):
                    j = jj * SUB + u
                    if it == 0:
                        lanes = pl.ds(pl.multiple_of(j * LANES, LANES), LANES)
                        v = x[:, lanes] + factor
                        p = tree(v, jnp.maximum)
                        e = jnp.exp(v - jnp.concatenate([p] * groups, axis=0))
                        held[j] = e
                        level[j] = p
                        partial[j] = tree(e, jnp.add)
                    else:
                        partial[j] = tree(held[j] * factor, jnp.add) * weight[j]
                return carry

            lax.fori_loop(c * per // SUB, (c + 1) * per // SUB, column_pass, 0)
            for g in range(c * per // SUB, (c + 1) * per // SUB):
                eight = pl.ds(g * SUB, SUB)
                s = [partial[eight, k, :] for k in range(SUB)]
                if it == 0:
                    p = [level[eight, k, :] for k in range(SUB)]
                    t = pairwise(p, jnp.maximum)
                    s = pairwise([s[k] * jnp.exp(p[k] - t) for k in range(SUB)], jnp.add)
                    mine[it, 0, eight, :] = t + jnp.log(s)
                else:
                    mine[it, 0, eight, :] = pairwise(s, jnp.add)
            tok_copy(it, 0, c).start()

        acc = jnp.zeros((experts, LANES), jnp.float32)
        for stage in range(stages):
            for c in range(chunks):
                tok_copy(it, stage, c).wait_recv()
                a, b = mine[it, stage, chunk(c), :], theirs[it, stage, chunk(c), :]
                if it == 0:
                    t = jnp.maximum(a, b)
                    joined = t + jnp.log(jnp.exp(a - t) + jnp.exp(b - t))
                else:
                    joined = a + b
                if stage < stages - 1:
                    mine[it, stage + 1, chunk(c), :] = joined
                    tok_copy(it, stage + 1, c).start()
                    continue
                if last:
                    tok_ref[chunk(c), :] = first_tok[chunk(c), :] - jnp.log(joined)
                    continue
                if it == 0:
                    first_tok[chunk(c), :] = -joined
                    scaled[chunk(c), :] = joined
                else:
                    scaled[chunk(c), :] = 1.0 / joined

                def row_pass(jj, acc):
                    for u in range(SUB):
                        j = jj * SUB + u
                        w = jnp.broadcast_to(scaled[pl.ds(j, 1), :], (SUB, LANES))
                        if it == 0:
                            w = jnp.exp(level[j] - w)
                            weight[j] = w
                        else:
                            w = weight[j] * w
                        acc = acc + held[j] * jnp.concatenate([w] * groups, axis=0)
                    return acc

                acc = lax.fori_loop(c * per // SUB, (c + 1) * per // SUB, row_pass, acc)
        if not last:
            parts = exchange_rows(it + 1, to_row(jnp.sum(acc, axis=1, keepdims=True)))
            total = functools.reduce(jnp.add, parts)
            factor = to_column(cap / total)
            if it == ITERS - 2:
                exp_ref[...] = first_exp + (log_cap - jnp.log(total))

    for it in range(ITERS):
        whole = rows_in.at[it]
        pltpu.make_async_copy(whole, whole, es_sem.at[it]).wait()
        for stage in range(stages):
            for c in range(chunks):
                tok_copy(it, stage, c).wait_send()


def solution(mesh):
    nx, nz, ny = mesh.shape["gx"], mesh.shape["gz"], mesh.shape["gy"]
    n = nx * nz
    stages = ny.bit_length() - 1
    chunks = 4

    def per_device(logits):
        experts, tokens = logits.shape
        blocks = tokens // LANES
        f32 = jnp.float32
        plane = pltpu.VMEM((blocks, LANES), f32)
        tok, exp = pl.pallas_call(
            functools.partial(kernel, nx, nz, ny, chunks),
            out_shape=(pltpu.VMEM((blocks, LANES), f32), pltpu.VMEM((1, LANES), f32)),
            in_specs=[pl.BlockSpec(memory_space=pl.ANY)],
            out_specs=(pl.BlockSpec(memory_space=pltpu.VMEM),) * 2,
            scratch_shapes=[
                pltpu.VMEM((experts, tokens), f32),
                pltpu.VMEM((experts, LANES), f32),
                pltpu.VMEM((experts, LANES), f32),
                pltpu.VMEM((ITERS, 1, LANES), f32),
                pltpu.VMEM((ITERS, n - 1, 1, LANES), f32),
                pltpu.VMEM((ITERS, stages, blocks, LANES), f32),
                pltpu.VMEM((ITERS, stages, blocks, LANES), f32),
                pltpu.VMEM((blocks, experts, LANES), f32),
                pltpu.VMEM((blocks, SUB, LANES), f32),
                pltpu.VMEM((blocks, SUB, LANES), f32),
                pltpu.VMEM((blocks, SUB, LANES), f32),
                plane, plane,
                pltpu.SemaphoreType.DMA((experts // SUB,)),
                pltpu.SemaphoreType.DMA((ITERS,)),
                pltpu.SemaphoreType.DMA((ITERS,)),
                pltpu.SemaphoreType.DMA((ITERS, stages, chunks)),
                pltpu.SemaphoreType.DMA((ITERS, stages, chunks)),
            ],
            compiler_params=pltpu.CompilerParams(
                collective_id=0, has_side_effects=True, vmem_limit_bytes=60 * 1024 * 1024),
        )(logits)
        return tok.reshape(tokens), exp[0, :experts]

    return jax.shard_map(
        per_device, mesh=mesh, in_specs=(P("gy", ("gx", "gz")),),
        out_specs=(P(("gx", "gz")), P("gy")), check_vma=False)
```

```python
import functools

import jax
import jax.numpy as jnp
from jax import lax
from jax.experimental import pallas as pl
from jax.experimental.pallas import tpu as pltpu
from jax.sharding import PartitionSpec as P

ITERS = 3
LANES = 128
SUB = 8
MESH = pl.DeviceIdType.MESH


def kernel(nx, nz, ny, chunks, x_hbm, tok_ref, exp_ref, x, y, tops, sums, rows_out, rows_in,
           mine, theirs, held, level, weight, partial, scaled, first_tok, factors, load_sem, move_sem, home_sem, es_sem, er_sem, ts_sem, tr_sem):
    experts, tokens = x.shape
    groups = experts // SUB
    half = tokens // 2
    blocks = half // LANES
    spots = nx * nz
    n = 2 * spots
    stages = ny.bit_length() - 2
    per = blocks // chunks
    gx, gz, gy = lax.axis_index("gx"), lax.axis_index("gz"), lax.axis_index("gy")
    core = lax.rem(gy, 2)
    me = (gx * nz + gz) * 2 + core
    cap = float(tokens * spots) / float(experts * ny)
    log_cap = jnp.log(jnp.full((1, LANES), cap, jnp.float32))

    loads = []
    for i in range(groups):
        rows = pl.ds(i * SUB, SUB)
        load = pltpu.make_async_copy(x_hbm.at[rows, :], x.at[rows, :], load_sem.at[i])
        load.start()
        loads.append(load)

    def peer(k):
        other = lax.rem(me + k, n)
        spot = other // 2
        return (spot // nz, lax.rem(spot, nz), gy - core + lax.rem(other, 2))

    def partner(stage):
        bit = 2 << stage
        up = lax.rem(gy // bit, 2)
        return (gx, gz, gy + bit - 2 * bit * up)

    sibling = (gx, gz, gy + 1 - 2 * core)

    barrier = pltpu.get_barrier_semaphore()

    def greet(k, carry):
        pl.semaphore_signal(barrier, inc=1, device_id=peer(k), device_id_type=MESH)
        return carry

    lax.fori_loop(1, n, greet, 0, unroll=n <= 16)
    for stage in range(stages):
        pl.semaphore_signal(barrier, inc=1, device_id=partner(stage), device_id_type=MESH)

    both = 2 * experts
    row_id = lax.broadcasted_iota(jnp.int32, (both, LANES), 0)
    lane_id = lax.broadcasted_iota(jnp.int32, (both, LANES), 1)
    diag = row_id == lane_id
    local_diag = row_id[:experts] + core * experts == lane_id[:experts]

    def to_row(column, where):
        return jnp.sum(jnp.where(where, jnp.broadcast_to(column, where.shape), 0.0),
                       axis=0, keepdims=True)

    def to_column(row):
        column = jnp.sum(jnp.where(diag, jnp.broadcast_to(row, (both, LANES)), 0.0),
                         axis=1, keepdims=True)
        return jnp.broadcast_to(column, (both, LANES))

    def exchange_rows(it, row):
        rows_out[it] = row

        def send(k, carry):
            pltpu.make_async_remote_copy(
                src_ref=rows_out.at[it], dst_ref=rows_in.at[it, k - 1],
                send_sem=es_sem.at[it], recv_sem=er_sem.at[it],
                device_id=peer(k), device_id_type=MESH).start()
            return carry

        lax.fori_loop(1, n, send, 0, unroll=n <= 16)
        whole = rows_in.at[it]
        pltpu.make_async_copy(whole, whole, er_sem.at[it]).wait()
        return [row] + [rows_in[it, k] for k in range(n - 1)]

    wide = 8 * LANES

    def pairwise(parts, combine):
        while len(parts) > 1:
            parts = [combine(*parts[k:k + 2]) if k + 1 < len(parts) else parts[k]
                     for k in range(0, len(parts), 2)]
        return parts[0]

    def fold(array, combine):
        return pairwise([array[:, k * LANES:(k + 1) * LANES]
                         for k in range(array.shape[1] // LANES)], combine)

    def tree(array, combine):
        return pairwise([array[k * SUB:(k + 1) * SUB] for k in range(array.shape[0] // SUB)], combine)

    for i in range(groups):
        rows = pl.ds(i * SUB, SUB)
        loads[i].wait()

        def higher(j, m):
            return jnp.maximum(m, x[rows, pl.ds(pl.multiple_of(j * wide, wide), wide)])

        m = fold(lax.fori_loop(1, tokens // wide, higher, x[rows, pl.ds(0, wide)], unroll=5),
                 jnp.maximum)
        tiled = jnp.concatenate([m] * 8, axis=1)

        def more(j, s):
            return s + jnp.exp(x[rows, pl.ds(pl.multiple_of(j * wide, wide), wide)] - tiled)

        s = fold(lax.fori_loop(0, tokens // wide, more, jnp.zeros((SUB, wide), jnp.float32),
                               unroll=4), jnp.add)
        tops[rows, :] = m
        sums[rows, :] = s

    lane_top = tops[...]
    top = jnp.max(lane_top, axis=1, keepdims=True)
    total = jnp.sum(sums[...] * jnp.exp(lane_top - top), axis=1, keepdims=True)
    local = jnp.where(lane_id[:1] // experts == core, to_row(top + jnp.log(total), local_diag), -1e30)

    pl.semaphore_wait(barrier, n - 1 + stages)

    away = pl.ds(pl.multiple_of((1 - core) * half, LANES), half)
    move = pltpu.make_async_remote_copy(
        src_ref=x.at[:, away], dst_ref=y, send_sem=move_sem.at[0], recv_sem=move_sem.at[1],
        device_id=sibling, device_id_type=MESH)
    move.start()
    parts = exchange_rows(0, local)
    top = functools.reduce(jnp.maximum, parts)
    total = functools.reduce(jnp.add, [jnp.exp(part - top) for part in parts])
    first_exp = log_cap - (top + jnp.log(total))
    factor = to_column(first_exp)
    factors[0] = factor[:experts]
    factors[1] = factor[experts:]
    move.wait_recv()

    def chunk(c):
        return pl.ds(c * per, per)

    def home_copy(c):
        rows = pl.ds(pl.multiple_of(core * blocks + c * per, SUB), per)
        return pltpu.make_async_remote_copy(
            src_ref=tok_ref.at[rows, :], dst_ref=tok_ref.at[rows, :],
            send_sem=home_sem.at[0, c], recv_sem=home_sem.at[1, c],
            device_id=sibling, device_id_type=MESH)

    def tok_copy(it, stage, c):
        return pltpu.make_async_remote_copy(
            src_ref=mine.at[it, stage, chunk(c), :], dst_ref=theirs.at[it, stage, chunk(c), :],
            send_sem=ts_sem.at[it, stage, c], recv_sem=tr_sem.at[it, stage, c],
            device_id=partner(stage), device_id_type=MESH)

    for it in range(ITERS):
        last = it == ITERS - 1
        for c in range(chunks):
            def column_pass(jj, carry):
                for u in range(SUB):
                    j = jj * SUB + u
                    if it == 0:
                        lanes = pl.ds(pl.multiple_of(core * half + j * LANES, LANES), LANES)
                        own = x[:, lanes] + factors[core]
                        other = (y[:, pl.ds(pl.multiple_of(j * LANES, LANES), LANES)]
                                 + factors[1 - core])
                        p = jnp.maximum(tree(own, jnp.maximum), tree(other, jnp.maximum))
                        tall = jnp.concatenate([p] * groups, axis=0)
                        own, other = jnp.exp(own - tall), jnp.exp(other - tall)
                        held[j, core] = own
                        held[j, 1 - core] = other
                        level[j] = p
                        partial[j] = tree(own, jnp.add) + tree(other, jnp.add)
                    else:
                        e = held[j].reshape(both, LANES) * factor
                        partial[j] = tree(e, jnp.add) * weight[j]
                return carry

            lax.fori_loop(c * per // SUB, (c + 1) * per // SUB, column_pass, 0)
            for g in range(c * per // SUB, (c + 1) * per // SUB):
                eight = pl.ds(g * SUB, SUB)
                s = [partial[eight, k, :] for k in range(SUB)]
                if it == 0:
                    p = [level[eight, k, :] for k in range(SUB)]
                    t = pairwise(p, jnp.maximum)
                    s = pairwise([s[k] * jnp.exp(p[k] - t) for k in range(SUB)], jnp.add)
                    mine[it, 0, eight, :] = t + jnp.log(s)
                else:
                    mine[it, 0, eight, :] = pairwise(s, jnp.add)
            tok_copy(it, 0, c).start()

        acc = jnp.zeros((both, LANES), jnp.float32)
        for stage in range(stages):
            for c in range(chunks):
                tok_copy(it, stage, c).wait_recv()
                a, b = mine[it, stage, chunk(c), :], theirs[it, stage, chunk(c), :]
                if it == 0:
                    t = jnp.maximum(a, b)
                    joined = t + jnp.log(jnp.exp(a - t) + jnp.exp(b - t))
                else:
                    joined = a + b
                if stage < stages - 1:
                    mine[it, stage + 1, chunk(c), :] = joined
                    tok_copy(it, stage + 1, c).start()
                    continue
                if last:
                    rows = pl.ds(pl.multiple_of(core * blocks + c * per, SUB), per)
                    tok_ref[rows, :] = first_tok[chunk(c), :] - jnp.log(joined)
                    home_copy(c).start()
                    continue
                if it == 0:
                    first_tok[chunk(c), :] = -joined
                    scaled[chunk(c), :] = joined
                else:
                    scaled[chunk(c), :] = 1.0 / joined

                def row_pass(jj, acc):
                    for u in range(SUB):
                        j = jj * SUB + u
                        w = jnp.broadcast_to(scaled[pl.ds(j, 1), :], (SUB, LANES))
                        if it == 0:
                            w = jnp.exp(level[j] - w)
                            weight[j] = w
                        else:
                            w = weight[j] * w
                        acc = acc + held[j].reshape(both, LANES) * jnp.concatenate([w] * (2 * groups), axis=0)
                    return acc

                acc = lax.fori_loop(c * per // SUB, (c + 1) * per // SUB, row_pass, acc)
        if not last:
            parts = exchange_rows(it + 1, to_row(jnp.sum(acc, axis=1, keepdims=True), diag))
            total = functools.reduce(jnp.add, parts)
            factor = to_column(cap / total)
            if it == ITERS - 2:
                final = first_exp + (log_cap - jnp.log(total))
                exp_ref[...] = jnp.where(core == 0, final[:, :experts], final[:, experts:both])

    for c in range(chunks):
        home_copy(c).wait()
    move.wait_send()
    for it in range(ITERS):
        whole = rows_in.at[it]
        pltpu.make_async_copy(whole, whole, es_sem.at[it]).wait()
        for stage in range(stages):
            for c in range(chunks):
                tok_copy(it, stage, c).wait_send()


def solution(mesh):
    nx, nz, ny = mesh.shape["gx"], mesh.shape["gz"], mesh.shape["gy"]
    n = 2 * nx * nz
    stages = ny.bit_length() - 2
    chunks = 2

    def per_device(logits):
        experts, tokens = logits.shape
        blocks = tokens // LANES // 2
        f32 = jnp.float32
        plane = pltpu.VMEM((blocks, LANES), f32)
        tok, exp = pl.pallas_call(
            functools.partial(kernel, nx, nz, ny, chunks),
            out_shape=(pltpu.VMEM((2 * blocks, LANES), f32), pltpu.VMEM((1, experts), f32)),
            in_specs=[pl.BlockSpec(memory_space=pl.ANY)],
            out_specs=(pl.BlockSpec(memory_space=pltpu.VMEM),) * 2,
            scratch_shapes=[
                pltpu.VMEM((experts, tokens), f32),
                pltpu.VMEM((experts, tokens // 2), f32),
                pltpu.VMEM((experts, LANES), f32),
                pltpu.VMEM((experts, LANES), f32),
                pltpu.VMEM((ITERS, 1, LANES), f32),
                pltpu.VMEM((ITERS, n - 1, 1, LANES), f32),
                pltpu.VMEM((ITERS, stages, blocks, LANES), f32),
                pltpu.VMEM((ITERS, stages, blocks, LANES), f32),
                pltpu.VMEM((blocks, 2, experts, LANES), f32),
                pltpu.VMEM((blocks, SUB, LANES), f32),
                pltpu.VMEM((blocks, SUB, LANES), f32),
                pltpu.VMEM((blocks, SUB, LANES), f32),
                plane, plane,
                pltpu.VMEM((2, experts, LANES), f32),
                pltpu.SemaphoreType.DMA((experts // SUB,)),
                pltpu.SemaphoreType.DMA((2,)),
                pltpu.SemaphoreType.DMA((2, chunks)),
                pltpu.SemaphoreType.DMA((ITERS,)),
                pltpu.SemaphoreType.DMA((ITERS,)),
                pltpu.SemaphoreType.DMA((ITERS, stages, chunks)),
                pltpu.SemaphoreType.DMA((ITERS, stages, chunks)),
            ],
            compiler_params=pltpu.CompilerParams(
                collective_id=0, has_side_effects=True, vmem_limit_bytes=60 * 1024 * 1024),
        )(logits)
        return tok.reshape(tokens), exp.reshape(experts)

    return jax.shard_map(
        per_device, mesh=mesh, in_specs=(P("gy", ("gx", "gz")),),
        out_specs=(P(("gx", "gz")), P("gy")), check_vma=False)
```
